32 devices in a mesh: seq: 16 (over z, y, x), tp: 2 (over core).
Axes of the slice: x: 2, y: 2, z: 4, core: 2. Of those that a mesh axis runs over, the one named last changes fastest.
Arguments:
- tokens: bfloat16 [8192, 2048], P('seq', 'tp'), may hold values from -6 to 6
- ln_gain: bfloat16 [2048], replicated, may hold values from 0.5 to 4.1
- w_qkv: bfloat16 [3, 2048, 2048], P(None, None, 'tp'), may hold values from -0.15467961 to 0.15467961
- w_out: bfloat16 [2048, 2048], P('tp'), may hold values from -0.1875 to 0.1875
Outputs:
- mixed: bfloat16 [8192, 2048], P('seq', 'tp')
The draws below stay inside these ranges and needn't reach their ends.
All inputs are finite; a program needn't handle non-finite values.
Results may differ from the reference program's by a relative error of at most 0.011.
Values may be sent and summed in bfloat16 or wider, within the bound.
A program may use at most 256 MiB of HBM per device.

```python
import jax
import jax.numpy as jnp
from jax import lax

D = 2048
HEADS = 16
HEAD_DIM = 128
SEQ = 8192


def draw_ln_gain(key, part):
    return jax.random.uniform(key, (D,), jnp.float32, 0.6, 1.4).astype(jnp.bfloat16)


def draw_tokens(key, part):
    normal_rows = jnp.clip(jax.random.normal(jax.random.fold_in(key, 11), (SEQ, D), jnp.float32), -6.0, 6.0)
    return normal_rows.astype(jnp.bfloat16)


def draw_w_qkv(key, part):
    bound_abs = 7.0 * D ** (-0.5)
    entries = jnp.clip(jax.random.normal(jax.random.fold_in(key, 23), (3, D, HEADS * HEAD_DIM), jnp.float32), -6.0, 6.0) * D ** (-0.5)
    return jnp.clip(entries, -bound_abs, bound_abs).astype(jnp.bfloat16)


def spiked(values, rng, source, target, parts, factor):
    def block_of(dim):
        return (jnp.arange(values.shape[dim]) // (values.shape[dim] // parts)).reshape((-1,) + (1,) * (values.ndim - 1 - dim))

    one_side = jax.random.permutation(rng, parts)[block_of(target)]
    other_side = (block_of(target) + parts // 2) % parts
    return jnp.where((block_of(source) == one_side) | (block_of(source) == other_side), factor * values, values)


def shard_levels(rng, shape, cuts, least, top_value):
    gain, own = 1.0, jax.random.fold_in(rng, 6)
    for axis_at, parts in cuts:
        draws = jnp.exp(jax.random.uniform(jax.random.fold_in(own, axis_at), (parts,), jnp.float32, least / len(cuts), top_value / len(cuts)))
        gain = gain * jnp.repeat(draws, shape[axis_at] // parts).reshape([-1 if axis == axis_at else 1 for axis in range(len(shape))])
    return gain


def gaussian_with(stream_key, shape, scale, most, split, heavy, kind=jnp.bfloat16):
    result = scale * jax.random.normal(stream_key, shape, jnp.float32)
    if split:
        result = result * shard_levels(stream_key, shape, split, -0.22, 0.18)
    return jnp.clip(spiked(result, jax.random.fold_in(stream_key, 3), *heavy), -most, most).astype(kind)


def setup_inputs(seed: int = 0) -> dict:
    seeds = jax.random.split(jax.random.key(seed), 5)
    return {
        "tokens": draw_tokens(jax.random.fold_in(seeds[4], 71), 0),
        "ln_gain": draw_ln_gain(jax.random.fold_in(seeds[4], 71), 0),
        "w_qkv": draw_w_qkv(jax.random.fold_in(seeds[4], 71), 0),
        "w_out": gaussian_with(seeds[3], (HEADS * HEAD_DIM, D), (HEADS * HEAD_DIM) ** -0.5, 0.1875, ((0, 2),), (0, 1, 2, 2.0)),
    }


def reference(tokens, ln_gain, w_qkv, w_out):
    values = tokens.astype(jnp.float32)
    average = lax.optimization_barrier(jnp.mean(values, axis=1, keepdims=True))
    second = lax.optimization_barrier(jnp.mean(values * values, axis=1, keepdims=True))
    normed = ((values - average) * lax.rsqrt(second - average * average + 1e-06) * ln_gain.astype(jnp.float32)).astype(jnp.bfloat16)
    queries = jnp.dot(normed, w_qkv[0], preferred_element_type=jnp.float32).astype(jnp.bfloat16).reshape(SEQ, HEADS, HEAD_DIM)
    keys_all = jnp.dot(normed, w_qkv[1], preferred_element_type=jnp.float32).astype(jnp.bfloat16).reshape(SEQ, HEADS, HEAD_DIM)
    vals_all = jnp.dot(normed, w_qkv[2], preferred_element_type=jnp.float32).astype(jnp.bfloat16).reshape(SEQ, HEADS, HEAD_DIM)
    span = min(512, SEQ)
    factor = HEAD_DIM ** (-0.5)
    keys_wide = keys_all.astype(jnp.float32)
    vals_wide = vals_all.astype(jnp.float32)

    def attend(offset):
        query_block = lax.dynamic_slice_in_dim(queries, offset, span, 0).astype(jnp.float32)
        scores = jnp.einsum('thc,shc->ths', query_block, keys_wide) * factor
        highest = lax.optimization_barrier(jnp.max(scores, axis=2, keepdims=True))
        expon = jnp.exp(scores - highest)
        denoms = lax.optimization_barrier(jnp.sum(expon, axis=2))
        weights = expon.astype(jnp.bfloat16).astype(jnp.float32)
        summed = jnp.einsum('ths,shc->thc', weights, vals_wide) / denoms[:, :, None]
        return summed.reshape(span, HEADS * HEAD_DIM).astype(jnp.bfloat16)
    offsets = jnp.arange(SEQ // span, dtype=jnp.int32) * span
    context = lax.map(attend, offsets).reshape(SEQ, HEADS * HEAD_DIM)
    projected = jnp.dot(context, w_out, preferred_element_type=jnp.float32)
    return (values + projected).astype(jnp.bfloat16)
```

```python
import functools
import math

import jax
import jax.numpy as jnp
from jax import lax
from jax.experimental import pallas as pl
from jax.experimental.pallas import tpu as pltpu
from jax.sharding import PartitionSpec as P

HEAD_DIM = 128
MESH = pl.DeviceIdType.MESH
ANY = pl.BlockSpec(memory_space=pl.ANY)


def remote(src, dst, send, recv, seq, tp):
    return pltpu.make_async_remote_copy(
        src_ref=src, dst_ref=dst, send_sem=send, recv_sem=recv, device_id=(seq, tp), device_id_type=MESH
    )


def put(src, dst, send, recv, seq, tp, own):
    @pl.when(own)
    def _():
        pltpu.make_async_copy(src, dst, recv).start()

    @pl.when(jnp.logical_not(own))
    def _():
        remote(src, dst, send, recv, seq, tp).start()


def half_kernel(
    n, heads, tok, gain, w_qkv, w_out, out,
    pair, far, normed, wbuf, wout, xq, xk, xv, yq, yk, yv, q_all, k_all, v_all, acc, top, s0, s1, ctx, held, sent, came, kept, res,
    lsem, swap, wsem, xsem, osem, qsend, qrecv, fsend, frecv, csend, crecv, psem,
):
    me, core = lax.axis_index("seq"), lax.axis_index("tp")
    other = 1 - core
    rows, feats = pair.shape[1], pair.shape[2]
    plane = n // 4
    near = n // 2
    piece = rows // plane
    layer, spot = me // plane, lax.rem(me, plane)
    side, inner = me // near, lax.rem(me // plane, 2)
    mate = (3 - layer) * plane + spot
    lane = lax.rem(me, 2)
    index = lax.rem(me, near) // 2
    head = side * plane + spot
    bf, f32 = jnp.bfloat16, jnp.float32

    mine = pltpu.make_async_copy(tok, pair.at[core], lsem.at[0])
    mine.start()
    trade = remote(tok, pair.at[core], swap.at[0], swap.at[1], me, other)
    trade.start()
    wide = 2 * HEAD_DIM
    groups = plane // 2

    def wcopy(b, j):
        at = pl.ds(pl.multiple_of(side * plane * HEAD_DIM + b * wide, wide), wide)
        return pltpu.make_async_copy(w_qkv.at[j, :, at], wbuf.at[b, j], wsem.at[b, j])

    for b in range(groups):
        for j in range(3):
            wcopy(b, j).start()
    fetch_out = pltpu.make_async_copy(w_out, wout, lsem.at[1])
    fetch_out.start()

    acc[...] = jnp.zeros_like(acc)
    top[...] = jnp.full_like(top, -1e30)
    v_all[:, HEAD_DIM:, :] = jnp.ones((v_all.shape[0], v_all.shape[1] - HEAD_DIM, v_all.shape[2]), bf)

    mine.wait()
    trade.wait()

    def part(ref, half, w):
        return ref.at[half, pl.ds(w * piece, piece)]

    def across(w, half):
        return remote(part(pair, half, w), part(far, half, w), xsem.at[0, w, half], xsem.at[1, w, half], mate, core)

    def inside(w, half):
        return remote(part(far, half, w), part(far, half, w), xsem.at[2, w, half], xsem.at[3, w, half], me, other)

    @pl.when(core == inner)
    def _():
        for w in range(plane):
            for half in range(2):
                across(w, half).start()

    step = 32

    def normalize(src, offset, count):
        def norm(i, carry):
            at = pl.ds(pl.multiple_of(offset + i * step, step), step)
            to = pl.ds(pl.multiple_of(i * step, step), step)
            a = src[0, at, :].astype(f32)
            b = src[1, at, :].astype(f32)
            average = (jnp.sum(a, axis=1, keepdims=True) + jnp.sum(b, axis=1, keepdims=True)) / (2 * feats)
            second = (jnp.sum(a * a, axis=1, keepdims=True) + jnp.sum(b * b, axis=1, keepdims=True)) / (2 * feats)
            scale = lax.rsqrt(second - average * average + 1e-06)
            normed[to, :feats] = ((a - average) * scale * gain[0:1, :feats]).astype(bf)
            normed[to, feats:] = ((b - average) * scale * gain[0:1, feats:]).astype(bf)
            return carry

        lax.fori_loop(0, count // step, norm, 0)

    factor = HEAD_DIM ** (-0.5) * math.log2(math.e)

    def deliver(block, h, pieces):
        chip = side * near + core * plane + h
        own = jnp.logical_and(chip == me, core == lane)
        for j, (src, dst) in enumerate(pieces):
            args = (src, dst, qsend.at[block, h, j], qrecv.at[block, index, j], chip, lane)
            put(*args, own)

    def delivered(block, h, pieces):
        chip = side * near + core * plane + h
        own = jnp.logical_and(chip == me, core == lane)

        @pl.when(jnp.logical_not(own))
        def _():
            for j, (src, dst) in enumerate(pieces):
                remote(src, dst, qsend.at[block, h, j], qrecv.at[block, index, j], chip, lane).wait_send()

    def spots(block, u, i):
        if block == 0:
            k_at = u * plane + i
            return q_all.at[i], k_all.at[k_at], v_all.at[k_at, pl.ds(0, HEAD_DIM)]
        k_at = 2 * plane + 2 * (block - 1) + u
        at = pl.ds(pl.multiple_of(i * piece, piece), piece)
        return q_all.at[plane + block - 1, at], k_all.at[k_at, at], v_all.at[k_at, pl.ds(0, HEAD_DIM), at]

    def staged(block, h):
        if block == 0:
            return xq.at[h], xk.at[h], xv.at[h]
        return yq.at[block - 1, h], yk.at[block - 1, h], yv.at[block - 1, h]

    def pieces_of(block, h):
        return list(zip(staged(block, h), spots(block, lane, index)))

    def project(block, count):
        for turn in range(groups):
            b = lax.rem(spot // 2 + turn, groups)
            for j in range(3):
                if block == 0:
                    wcopy(b, j).wait()
                got = jnp.dot(normed[:count, :], wbuf[b, j], preferred_element_type=f32)
                if j == 0:
                    got = got * factor
                for half in range(2):
                    cut = got[:, half * HEAD_DIM : (half + 1) * HEAD_DIM]
                    store = staged(block, 2 * b + half)[j]
                    store[...] = (cut.T if j == 2 else cut).astype(bf)
            for half in range(2):
                h = 2 * b + lax.rem(spot + half, 2)
                deliver(block, h, pieces_of(block, h))

    def wave(w):
        @pl.when(core != inner)
        def _():
            for half in range(2):
                across(w, half).wait_recv()
                inside(w, half).start()

        @pl.when(core == inner)
        def _():
            for half in range(2):
                inside(w, half).wait_recv()

        normalize(far, w * piece, piece)
        project(w + 1, piece)

    def wait_block(block, i):
        for j, (src, dst) in enumerate(zip(staged(block, 0), spots(block, core, i))):
            remote(src, dst, qsend.at[block, 0, j], qrecv.at[block, i, j], me, other).wait_recv()

    def share(slot, u, way):
        at = u * plane + slot if way == 0 else 2 * plane + 2 * slot + u
        sem = slot if way == 0 else plane + slot
        return (
            remote(k_all.at[at], k_all.at[at], fsend.at[sem, 0], frecv.at[sem, 0], me, other),
            remote(
                v_all.at[at, pl.ds(0, HEAD_DIM)], v_all.at[at, pl.ds(0, HEAD_DIM)], fsend.at[sem, 1], frecv.at[sem, 1], me, other
            ),
        )

    def pass_on(slot, way):
        for copy in share(slot, core, way):
            copy.start()

    def from_other(slot, way):
        for copy in share(slot, other, way):
            copy.wait_recv()

    def segment(rects):
        total = sum(nq * nk for _, nq, _, nk in rects)

        def find(t):
            spot_q = spot_k = None
            before = 0
            for q0, nq, k0, nk in rects:
                a = q0 + (t - before) // nk
                b = k0 + lax.rem(t - before, nk)
                if spot_q is None:
                    spot_q, spot_k = a, b
                else:
                    spot_q = jnp.where(t >= before, a, spot_q)
                    spot_k = jnp.where(t >= before, b, spot_k)
                before += nq * nk
            return spot_q, spot_k

        def score(t, s):
            a, b = find(t)
            s[...] = lax.dot_general(k_all[b], q_all[a], (((1,), (1,)), ((), ())), preferred_element_type=f32)

        def weigh(t, s):
            a, b = find(t)
            now = s[...]
            was = top[a]
            high = jnp.maximum(was, jnp.max(now, axis=0, keepdims=True))
            p = jnp.exp2((now - high).astype(bf))
            add = jnp.dot(v_all[b], p, preferred_element_type=f32)
            acc[a] = acc[a] * jnp.exp2(was - high) + add
            top[a] = high

        score(jnp.int32(0), s0)

        def body(i, carry):
            t = 2 * i
            score(t + 1, s1)
            weigh(t, s0)
            score(jnp.minimum(t + 2, total - 1), s0)
            weigh(t + 1, s1)
            return carry

        lax.fori_loop(0, total // 2, body, 0)
        if total % 2:
            weigh(jnp.int32(total - 1), s0)

    def place(l, at):
        return held.at[at, pl.ds(pl.multiple_of(l * HEAD_DIM, HEAD_DIM), HEAD_DIM)]

    def returns(b):
        if b < plane:
            s = side * near + 2 * b + core
            own = jnp.logical_and(s == me, inner == core)
            return [((ctx.at[b], place(head, pl.ds(0, rows)), csend.at[b, 0], crecv.at[head, 0], s, inner), own)]
        w = b - plane
        found = []
        for i in range(plane):
            s = side * near + 2 * i + core
            owner = (3 - s // plane) * plane + lax.rem(s, plane)
            src = ctx.at[b, pl.ds(i * piece, piece)]
            found.append(((src, place(head, pl.ds(w * piece, piece)), csend.at[b, i], crecv.at[head, w], owner, inner), None))
        return found

    def finish(first, count):
        def one(b, carry):
            t = acc[b]
            ctx[b] = (t[:HEAD_DIM] / t[HEAD_DIM : HEAD_DIM + 1]).T.astype(bf)
            return carry

        lax.fori_loop(first, first + count, one, 0)
        for b in range(first, first + count):
            for args, own in returns(b):
                if own is None:
                    remote(*args).start()
                else:
                    put(*args, own)

    normalize(pair, 0, rows)
    project(0, rows)
    wave(0)
    here, there = 2 * inner, 2 * (1 - inner)
    for k in range(2):
        wait_block(0, here + k)
        pass_on(here + k, 0)
    segment([(here, 2, core * plane + here, 2)])
    for k in range(2):
        wait_block(0, there + k)
        pass_on(there + k, 0)
    segment([(here, 2, core * plane + there, 2), (there, 2, core * plane, plane)])
    wave(1)
    for k in range(plane):
        from_other(k, 0)
    segment([(0, plane, other * plane, plane)])

    def take(w):
        for i in range(plane):
            wait_block(w + 1, i)
        pass_on(w, 1)

    for w in range(plane):
        fresh, old = plane + w, 2 * plane + 2 * w
        take(w)
        if w < plane - 1:
            segment([(0, fresh, old + core, 1), (fresh, 1, 0, old), (fresh, 1, old + core, 1)])
            if w + 2 < plane:
                wave(w + 2)
            from_other(w, 1)
            segment([(0, fresh + 1, old + other, 1)])
        else:
            segment([(0, fresh, old + core, 1)])
            from_other(w, 1)
            segment([(plane, plane - 1, old + other, 1)])
            finish(plane, plane - 1)
            segment([(fresh, 1, 0, old + 2)])
            finish(fresh, 1)
            segment([(0, plane, old + other, 1)])
            finish(0, plane)

    fetch_out.wait()
    for k in range(plane):
        l = side * plane + k
        remote(ctx.at[0], place(l, pl.ds(0, rows)), csend.at[0, 0], crecv.at[l, 0], me, other).wait_recv()

    def product(half, w):
        at = pl.ds(pl.multiple_of(half * feats, feats), feats)
        return jnp.dot(held[w * piece : (w + 1) * piece, :], wout[:, at], preferred_element_type=f32)

    def hand(w):
        return remote(sent.at[w], came.at[w], psem.at[0, w], psem.at[1, w], me, other)

    def leave(w):
        at = pl.ds(w * piece, piece)
        return pltpu.make_async_copy(res.at[at], out.at[at], osem.at[w])

    for w in range(plane):
        for k in range(plane):
            l = (1 - side) * plane + k
            at = pl.ds(w * piece, piece)
            remote(ctx.at[0, at], place(l, at), csend.at[0, 0], crecv.at[l, w], me, other).wait_recv()
        sent[w] = product(other, w).astype(bf)
        hand(w).start()
        kept[w * piece : (w + 1) * piece, :] = product(core, w)

    for w in range(plane):
        hand(w).wait_recv()
        at = slice(w * piece, (w + 1) * piece)
        res[at, :] = (pair[core, at, :].astype(f32) + (kept[at, :] + came[w].astype(f32))).astype(bf)
        leave(w).start()

    for block in range(plane + 1):
        for h in range(plane):
            delivered(block, h, pieces_of(block, h))
    for slot in range(plane):
        for way in range(2):
            for copy in share(slot, core, way):
                copy.wait_send()

    @pl.when(core == inner)
    def _():
        for w in range(plane):
            for half in range(2):
                across(w, half).wait_send()

    @pl.when(core != inner)
    def _():
        for w in range(plane):
            for half in range(2):
                inside(w, half).wait_send()

    for b in range(2 * plane):
        for args, own in returns(b):
            if own is None:
                remote(*args).wait_send()
            else:

                @pl.when(jnp.logical_not(own))
                def _():
                    remote(*args).wait_send()

    for w in range(plane):
        hand(w).wait_send()
        leave(w).wait()


def half_per_layer(n, tokens, ln_gain, w_qkv, w_out):
    rows, feats = tokens.shape
    heads = w_qkv.shape[2] // HEAD_DIM
    plane = n // 4
    piece = rows // plane
    bf, f32 = jnp.bfloat16, jnp.float32
    dma = pltpu.SemaphoreType.DMA
    gain = ln_gain.astype(f32).reshape(1, -1)
    chunks = 4 * plane
    blocks = 2 * plane
    extra = HEAD_DIM + 16
    vmem = pltpu.VMEM
    return pl.pallas_call(
        functools.partial(half_kernel, n, heads),
        out_shape=jax.ShapeDtypeStruct((rows, feats), bf),
        in_specs=[ANY, pl.BlockSpec(memory_space=pltpu.VMEM), ANY, ANY],
        out_specs=ANY,
        scratch_shapes=[
            vmem((2, rows, feats), bf),
            vmem((2, rows, feats), bf),
            vmem((rows, 2 * feats), bf),
            vmem((plane // 2, 3, 2 * feats, 2 * HEAD_DIM), bf),
            vmem(w_out.shape, bf),
            vmem((plane, rows, HEAD_DIM), bf),
            vmem((plane, rows, HEAD_DIM), bf),
            vmem((plane, HEAD_DIM, rows), bf),
            vmem((plane, plane, piece, HEAD_DIM), bf),
            vmem((plane, plane, piece, HEAD_DIM), bf),
            vmem((plane, plane, HEAD_DIM, piece), bf),
            vmem((blocks, rows, HEAD_DIM), bf),
            vmem((chunks, rows, HEAD_DIM), bf),
            vmem((chunks, extra, rows), bf),
            vmem((blocks, extra, rows), f32),
            vmem((blocks, 1, rows), f32),
            vmem((rows, rows), f32),
            vmem((rows, rows), f32),
            vmem((blocks, rows, HEAD_DIM), bf),
            vmem((rows, heads * HEAD_DIM), bf),
            vmem((plane, piece, feats), bf),
            vmem((plane, piece, feats), bf),
            vmem((rows, feats), f32),
            vmem((rows, feats), bf),
            dma((2,)), dma((2,)), dma((plane // 2, 3)), dma((4, plane, 2)), dma((plane,)),
            dma((plane + 1, plane, 3)), dma((plane + 1, plane, 3)), dma((blocks, 2)), dma((blocks, 2)),
            dma((blocks, plane)), dma((heads, plane)), dma((2, plane)),
        ],
        compiler_params=pltpu.CompilerParams(has_side_effects=True, vmem_limit_bytes=60 * 1024 * 1024),
        name="sublayer",
    )(tokens, gain, w_qkv, w_out)


def attend_block(totals, queries, block_kv, factor):
    running, denoms, accum = totals
    heads_here = queries.shape[1]
    keys_part = block_kv[0].reshape(block_kv.shape[1], heads_here, queries.shape[2])
    vals_part = block_kv[1].reshape(block_kv.shape[1], heads_here, queries.shape[2])
    scores = (
        jnp.einsum("thc,shc->ths", queries, keys_part, preferred_element_type=jnp.float32) * factor
    )
    highest = jnp.maximum(running, jnp.max(scores, axis=2))
    expon = jnp.exp(scores - highest[:, :, None])
    denoms = jnp.sum(expon, axis=2)
    weights = expon.astype(jnp.bfloat16)
    accum = jnp.einsum("ths,shc->thc", weights, vals_part, preferred_element_type=jnp.float32)
    return (highest, denoms, accum)


def start_totals(rows, heads_count):
    return (
        jnp.full((rows, heads_count), -1e30, jnp.float32),
        jnp.zeros((rows, heads_count), jnp.float32),
        jnp.zeros((rows, heads_count, HEAD_DIM), jnp.float32),
    )


def on_device(tokens, ln_gain, w_qkv, w_out):
    tok_rows = tokens.shape[0]
    whole = lax.all_gather(tokens, "tp", axis=1, tiled=True)
    values = whole.astype(jnp.float32)
    average = jnp.mean(values, axis=1, keepdims=True)
    second = jnp.mean(values * values, axis=1, keepdims=True)
    normed = (
        (values - average)
        * lax.rsqrt(second - average * average + 1e-06)
        * ln_gain.astype(jnp.float32)
    ).astype(jnp.bfloat16)
    projected = jnp.einsum("td,jdc->jtc", normed, w_qkv, preferred_element_type=jnp.float32).astype(
        jnp.bfloat16
    )
    heads_here = w_qkv.shape[2] // HEAD_DIM
    factor = HEAD_DIM ** (-0.5)
    queries = projected[0].reshape(tok_rows, heads_here, HEAD_DIM)
    keys_vals = projected[1:3]
    initial = start_totals(tok_rows, heads_here)
    final = attend_block(
        initial, queries, lax.all_gather(keys_vals, "seq", axis=1, tiled=True), factor
    )
    context = (
        (final[2] / final[1][:, :, None])
        .reshape(tok_rows, heads_here * HEAD_DIM)
        .astype(jnp.bfloat16)
    )
    summed = lax.psum_scatter(
        lax.dot_general(
            w_out, context, (((0,), (1,)), ((), ())), preferred_element_type=jnp.float32
        ).astype(jnp.bfloat16),
        "tp",
        scatter_dimension=0,
        tiled=True,
    ).astype(jnp.float32)
    return (tokens.astype(jnp.float32) + summed.T).astype(jnp.bfloat16)


def solution(mesh):
    in_specs = (P("seq", "tp"), P(), P(None, None, "tp"), P("tp", None))
    out_specs = P("seq", "tp")
    n, cores = mesh.shape["seq"], mesh.shape["tp"]

    def run(tokens, ln_gain, w_qkv, w_out):
        heads = w_qkv.shape[2] // HEAD_DIM
        if cores == 2 and heads * cores == n and n % 8 == 0 and tokens.shape[0] % n == 0:
            return half_per_layer(n, tokens, ln_gain, w_qkv, w_out)
        return on_device(tokens, ln_gain, w_qkv, w_out)

    return jax.shard_map(run, mesh=mesh, in_specs=in_specs, out_specs=out_specs, check_vma=False)
```

```python
import functools
import math

import jax
import jax.numpy as jnp
from jax import lax
from jax.experimental import pallas as pl
from jax.experimental.pallas import tpu as pltpu
from jax.sharding import PartitionSpec as P

HEAD_DIM = 128
MESH = pl.DeviceIdType.MESH


def remote(src, dst, send, recv, seq, tp):
    return pltpu.make_async_remote_copy(
        src_ref=src, dst_ref=dst, send_sem=send, recv_sem=recv, device_id=(seq, tp), device_id_type=MESH
    )


def put(src, dst, send, recv, seq, tp, own):
    @pl.when(own)
    def _():
        pltpu.make_async_copy(src, dst, recv).start()

    @pl.when(jnp.logical_not(own))
    def _():
        remote(src, dst, send, recv, seq, tp).start()


def barrier_wait(barrier, count):
    pl.semaphore_wait(barrier, count)


def half_kernel(
    n, heads, tok, gain_ref, w_qkv, w_out, out,
    pair, far, normed, first, wbuf, wout, xq, xk, xv, yq, yk, yv, q_all, k_all, v_all, acc, top, s0, s1, ctx, held, sent, came,
    kept, res, gain, lsem, swap, wsem, xsem, osem, qsend, qrecv, fsend, frecv, csend, crecv, psem,
):
    me, core = lax.axis_index("seq"), lax.axis_index("tp")
    other = 1 - core
    rows, feats = pair.shape[1], pair.shape[2]
    plane, near = n // 4, n // 2
    groups = plane // 2
    piece = rows // groups
    layer, spot = me // plane, lax.rem(me, plane)
    side, inner = me // near, lax.rem(me // plane, 2)
    central = inner != side
    mate = (2 - side) * plane + spot
    lane = lax.rem(me, 2)
    head = side * plane + spot
    bf, f32 = jnp.bfloat16, jnp.float32

    barrier = pltpu.get_barrier_semaphore()

    def greet(i, carry):
        there = lax.rem(2 * me + core + i, 2 * n)
        pl.semaphore_signal(barrier, inc=1, device_id=(there // 2, lax.rem(there, 2)), device_id_type=MESH)
        return carry

    lax.fori_loop(1, 2 * n, greet, 0)
    mine = pltpu.make_async_copy(tok, pair.at[core], lsem.at[0])
    mine.start()
    trade = remote(tok, pair.at[core], swap.at[0], swap.at[1], me, other)

    def cut(c):
        return pl.ds(c * piece, piece)

    kind = 1 - central.astype(jnp.int32)

    def across(c, half, src=None):
        src = normed.at[half, cut(c)] if src is None else src
        return remote(src, far.at[kind, half, cut(c)], xsem.at[0, kind, c, half], xsem.at[1, kind, c, half], mate, core)

    def inside(which, c, half):
        ref = far.at[which, half, cut(c)]
        return remote(ref, ref, xsem.at[2, which, c, half], xsem.at[3, which, c, half], me, other)

    def sends_x(when):
        return jnp.logical_and(core == inner, when)

    def wcopy(j):
        at = pl.ds(pl.multiple_of(side * plane * HEAD_DIM, HEAD_DIM), plane * HEAD_DIM)
        return pltpu.make_async_copy(w_qkv.at[j, :, at], wbuf.at[j], wsem.at[j])

    for j in range(3):
        wcopy(j).start()
    fetch_out = pltpu.make_async_copy(w_out, wout, lsem.at[1])
    fetch_out.start()
    gain[...] = gain_ref[...].astype(f32).reshape(1, 2 * feats)
    acc[...] = jnp.zeros_like(acc)
    top[...] = jnp.full_like(top, -1e30)
    v_all[:, HEAD_DIM:, :] = jnp.ones((v_all.shape[0], v_all.shape[1] - HEAD_DIM, v_all.shape[2]), bf)
    barrier_wait(barrier, 2 * n - 1)
    trade.start()

    @pl.when(sends_x(central))
    def _():
        across(0, core, tok.at[cut(0)]).start()

    mine.wait()
    trade.wait()

    @pl.when(sends_x(central))
    def _():
        across(0, other, pair.at[other, cut(0)]).start()

    step = 32

    def normalize(src, dst, count):
        def norm(i, carry):
            to = pl.ds(pl.multiple_of(i * step, step), step)
            a = src[0, to, :].astype(f32)
            b = src[1, to, :].astype(f32)
            average = (jnp.sum(a, axis=1, keepdims=True) + jnp.sum(b, axis=1, keepdims=True)) / (2 * feats)
            second = (jnp.sum(a * a, axis=1, keepdims=True) + jnp.sum(b * b, axis=1, keepdims=True)) / (2 * feats)
            scale = lax.rsqrt(second - average * average + 1e-06)
            dst[0, to, :] = ((a - average) * scale * gain[0:1, :feats]).astype(bf)
            dst[1, to, :] = ((b - average) * scale * gain[0:1, feats:]).astype(bf)
            return carry

        lax.fori_loop(0, count // step, norm, 0)

    factor = HEAD_DIM ** (-0.5) * math.log2(math.e)

    def spots(block, u, i):
        if block == 0:
            k_at = u * plane + i
            return q_all.at[i], k_all.at[k_at], v_all.at[k_at, pl.ds(0, HEAD_DIM)]
        k_at = 2 * plane + 2 * (block - 1) + u
        at = pl.ds(pl.multiple_of(i * piece, piece), piece)
        return q_all.at[plane + block - 1, at], k_all.at[k_at, at], v_all.at[k_at, pl.ds(0, HEAD_DIM), at]

    def staged(block, h):
        if block == 0:
            return xq.at[h], xk.at[h], xv.at[h]
        return yq.at[block - 1, h], yk.at[block - 1, h], yv.at[block - 1, h]

    def moves(block, h, j):
        chip = side * near + core * plane + h
        own = jnp.logical_and(chip == me, core == lane)
        i = lax.rem(me, near) // 2 if block == 0 else spot // 2
        src, dst = staged(block, h)[j], spots(block, lane, i)[j]
        return (src, dst, qsend.at[block, h, j], qrecv.at[block, i, j], chip, lane), own

    def deliver(block, h, j):
        args, own = moves(block, h, j)
        put(*args, own)

    def delivered(block, h, j):
        args, own = moves(block, h, j)

        @pl.when(jnp.logical_not(own))
        def _():
            remote(*args).wait_send()

    def project(block, src):
        for j in range(3):
            if block == 0:
                wcopy(j).wait()
            got = jnp.dot(src[0], wbuf[j, :feats], preferred_element_type=f32)
            got = got + jnp.dot(src[1], wbuf[j, feats:], preferred_element_type=f32)
            if j == 0:
                got = got * factor
            for h in range(plane):
                part = got[:, h * HEAD_DIM : (h + 1) * HEAD_DIM]
                staged(block, h)[j][...] = (part.T if j == 2 else part).astype(bf)
            for turn in range(plane):
                deliver(block, lax.rem(spot + turn, plane), j)

    def wave(w):
        which, c = w // groups, w % groups

        @pl.when(central)
        def _():
            lands = core == (side if which == 0 else 1 - side)

            @pl.when(lands)
            def _():
                for half in range(2):
                    ref = far.at[which, half, cut(c)]
                    remote(ref, ref, xsem.at[0, which, c, half], xsem.at[1, which, c, half], mate, core).wait_recv()
                    inside(which, c, half).start()

            @pl.when(jnp.logical_not(lands))
            def _():
                for half in range(2):
                    inside(which, c, half).wait_recv()

            if w == 0:
                normalize(far.at[0, :, cut(0)], first, piece)
                project(1, first)
            else:
                project(w + 1, far.at[which, :, cut(c)])

    def wait_block(block, i):
        for j, (src, dst) in enumerate(zip(staged(block, 0), spots(block, core, i))):
            remote(src, dst, qsend.at[block, 0, j], qrecv.at[block, i, j], me, other).wait_recv()

    def share(slot, u, way):
        at = u * plane + slot if way == 0 else 2 * plane + 2 * slot + u
        sem = slot if way == 0 else plane + slot
        k_ref, v_ref = k_all.at[at], v_all.at[at, pl.ds(0, HEAD_DIM)]
        return (
            remote(k_ref, k_ref, fsend.at[sem, 0], frecv.at[sem, 0], me, other),
            remote(v_ref, v_ref, fsend.at[sem, 1], frecv.at[sem, 1], me, other),
        )

    def pass_on(slot, way):
        for copy in share(slot, core, way):
            copy.start()

    def from_other(slot, way):
        for copy in share(slot, other, way):
            copy.wait_recv()

    def segment(rects):
        total = sum(nq * nk for _, nq, _, nk in rects)

        def find(t):
            spot_q = spot_k = None
            before = 0
            for q0, nq, k0, nk in rects:
                a = q0 + (t - before) // nk
                b = k0 + lax.rem(t - before, nk)
                if spot_q is None:
                    spot_q, spot_k = a, b
                else:
                    spot_q = jnp.where(t >= before, a, spot_q)
                    spot_k = jnp.where(t >= before, b, spot_k)
                before += nq * nk
            return spot_q, spot_k

        def score(t, s):
            a, b = find(t)
            s[...] = lax.dot_general(k_all[b], q_all[a], (((1,), (1,)), ((), ())), preferred_element_type=f32)

        def weigh(t, s):
            a, b = find(t)
            now = s[...]
            was = top[a]
            high = jnp.maximum(was, jnp.max(now, axis=0, keepdims=True))
            p = jnp.exp2((now - high).astype(bf))
            add = jnp.dot(v_all[b], p, preferred_element_type=f32)
            acc[a] = acc[a] * jnp.exp2(was - high) + add
            top[a] = high

        score(jnp.int32(0), s0)

        def body(i, carry):
            t = 2 * i
            score(t + 1, s1)
            weigh(t, s0)
            score(jnp.minimum(t + 2, total - 1), s0)
            weigh(t + 1, s1)
            return carry

        lax.fori_loop(0, total // 2, body, 0)
        if total % 2:
            weigh(jnp.int32(total - 1), s0)

    def place(l, at):
        return held.at[at, pl.ds(pl.multiple_of(l * HEAD_DIM, HEAD_DIM), HEAD_DIM)]

    def returns(b):
        if b < plane:
            s = side * near + 2 * b + core
            own = jnp.logical_and(s == me, inner == core)
            return [((ctx.at[b], place(head, pl.ds(0, rows)), csend.at[b, 0], crecv.at[head, 0], s, inner), own)]
        w = b - plane
        which, c = w // groups, w % groups
        home = (2 - side) if which == 0 else 3 * (1 - side)
        return [
            ((ctx.at[b, cut(i)], place(head, cut(c)), csend.at[b, i], crecv.at[head, c], home * plane + 2 * i + core, inner), None)
            for i in range(groups)
        ]

    def finish(start, count):
        def one(b, carry):
            t = acc[b]
            ctx[b] = (t[:HEAD_DIM] / t[HEAD_DIM : HEAD_DIM + 1]).T.astype(bf)
            return carry

        lax.fori_loop(start, start + count, one, 0)
        for b in range(start, start + count):
            for args, own in returns(b):
                if own is None:
                    remote(*args).start()
                else:
                    put(*args, own)

    normalize(pair, normed, rows)

    @pl.when(sends_x(central))
    def _():
        for c in range(1, groups):
            for half in range(2):
                across(c, half).start()

    project(0, normed)

    wave(0)
    here, there = groups * inner, groups * (1 - inner)
    for k in range(groups):
        wait_block(0, here + k)
        pass_on(here + k, 0)

    @pl.when(sends_x(jnp.logical_not(central)))
    def _():
        for c in range(groups):
            for half in range(2):
                across(c, half).start()

    segment([(here, groups, core * plane + here, groups)])
    wave(1)
    for k in range(groups):
        wait_block(0, there + k)
        pass_on(there + k, 0)
    segment([(here, groups, core * plane + there, groups), (there, groups, core * plane, plane)])
    for k in range(plane):
        from_other(k, 0)
    segment([(0, plane, other * plane, plane)])
    wave(2)

    def take(w):
        for i in range(groups):
            wait_block(w + 1, i)
        pass_on(w, 1)

    base = 2 * plane
    take(0)
    segment([(plane, 1, 0, base)])
    from_other(0, 1)
    segment([(plane, 1, base, 2), (0, plane, base, 2)])
    wave(3)
    take(1)
    segment([(plane + 1, 1, 0, base + 2), (plane, 2, base + 2 + core, 1)])
    from_other(1, 1)
    segment([(plane, 2, base + 2 + other, 1), (0, plane, base + 2, 2)])
    take(2)
    segment([(plane + 2, 1, 0, base + 4), (plane, 3, base + 4 + core, 1)])
    from_other(2, 1)
    take(3)
    segment([(plane, 3, base + 4 + other, 1), (plane, 3, base + 6 + core, 1)])
    from_other(3, 1)
    segment([(plane, 3, base + 6 + other, 1)])
    finish(plane, plane - 1)
    segment([(plane + 3, 1, 0, base + 8)])
    finish(plane + 3, 1)
    for half in range(2):
        segment([(half * groups, groups, base + 4, 4)])
        finish(half * groups, groups)

    fetch_out.wait()
    for k in range(plane):
        l = side * plane + k
        remote(ctx.at[0], place(l, pl.ds(0, rows)), csend.at[0, 0], crecv.at[l, 0], me, other).wait_recv()

    def product(half, c):
        at = pl.ds(pl.multiple_of(half * feats, feats), feats)
        return jnp.dot(held[c * piece : (c + 1) * piece, :], wout[:, at], preferred_element_type=f32)

    def hand(c):
        return remote(sent.at[c], came.at[c], psem.at[0, c], psem.at[1, c], me, other)

    def leave(c):
        return pltpu.make_async_copy(res.at[cut(c)], out.at[cut(c)], osem.at[c])

    for c in range(groups):
        for k in range(plane):
            l = (1 - side) * plane + k
            remote(ctx.at[0, cut(c)], place(l, cut(c)), csend.at[0, 0], crecv.at[l, c], me, other).wait_recv()
        sent[c] = product(other, c).astype(bf)
        hand(c).start()
        kept[c * piece : (c + 1) * piece, :] = product(core, c)

    for c in range(groups):
        hand(c).wait_recv()
        at = slice(c * piece, (c + 1) * piece)
        res[at, :] = (pair[core, at, :].astype(f32) + (kept[at, :] + came[c].astype(f32))).astype(bf)
        leave(c).start()

    for h in range(plane):
        for j in range(3):
            delivered(0, h, j)

    @pl.when(central)
    def _():
        for block in range(1, plane + 1):
            for h in range(plane):
                for j in range(3):
                    delivered(block, h, j)
        for which in range(2):
            lands = core == (side if which == 0 else 1 - side)

            @pl.when(lands)
            def _():
                for c in range(groups):
                    for half in range(2):
                        inside(which, c, half).wait_send()

    for slot in range(plane):
        for way in range(2):
            for copy in share(slot, core, way):
                copy.wait_send()

    @pl.when(core == inner)
    def _():
        for c in range(groups):
            for half in range(2):
                across(c, half).wait_send()

    for b in range(2 * plane):
        for args, own in returns(b):
            if own is None:
                remote(*args).wait_send()
            else:

                @pl.when(jnp.logical_not(own))
                def _():
                    remote(*args).wait_send()

    for c in range(groups):
        hand(c).wait_send()
        leave(c).wait()


def half_per_layer(n, tokens, ln_gain, w_qkv, w_out):
    rows, feats = tokens.shape
    heads = w_qkv.shape[2] // HEAD_DIM
    plane = n // 4
    groups = plane // 2
    piece = rows // groups
    bf, f32 = jnp.bfloat16, jnp.float32
    dma = pltpu.SemaphoreType.DMA
    chunks, blocks = 4 * plane, 2 * plane
    extra = HEAD_DIM + 16
    vmem = pltpu.VMEM
    hbm = pl.BlockSpec(memory_space=pltpu.HBM)
    return pl.pallas_call(
        functools.partial(half_kernel, n, heads),
        out_shape=jax.ShapeDtypeStruct((rows, feats), bf),
        in_specs=[hbm, pl.BlockSpec(memory_space=pltpu.VMEM), hbm, hbm],
        out_specs=hbm,
        scratch_shapes=[
            vmem((2, rows, feats), bf),
            vmem((2, 2, rows, feats), bf),
            vmem((2, rows, feats), bf),
            vmem((2, piece, feats), bf),
            vmem((3, 2 * feats, plane * HEAD_DIM), bf),
            vmem(w_out.shape, bf),
            vmem((plane, rows, HEAD_DIM), bf),
            vmem((plane, rows, HEAD_DIM), bf),
            vmem((plane, HEAD_DIM, rows), bf),
            vmem((plane, plane, piece, HEAD_DIM), bf),
            vmem((plane, plane, piece, HEAD_DIM), bf),
            vmem((plane, plane, HEAD_DIM, piece), bf),
            vmem((blocks, rows, HEAD_DIM), bf),
            vmem((chunks, rows, HEAD_DIM), bf),
            vmem((chunks, extra, rows), bf),
            vmem((blocks, extra, rows), f32),
            vmem((blocks, 1, rows), f32),
            vmem((rows, rows), f32),
            vmem((rows, rows), f32),
            vmem((blocks, rows, HEAD_DIM), bf),
            vmem((rows, heads * HEAD_DIM), bf),
            vmem((groups, piece, feats), bf),
            vmem((groups, piece, feats), bf),
            vmem((rows, feats), f32),
            vmem((rows, feats), bf),
            vmem((1, 2 * feats), f32),
            dma((2,)), dma((2,)), dma((3,)), dma((4, 2, groups, 2)), dma((groups,)),
            dma((plane + 1, plane, 3)), dma((plane + 1, plane, 3)), dma((blocks, 2)), dma((blocks, 2)),
            dma((blocks, groups)), dma((heads, groups)), dma((2, groups)),
        ],
        compiler_params=pltpu.CompilerParams(collective_id=0, has_side_effects=True, vmem_limit_bytes=60 * 1024 * 1024),
        name="sublayer",
    )(tokens, ln_gain, w_qkv, w_out)


def attend_block(totals, queries, block_kv, factor):
    running, denoms, accum = totals
    heads_here = queries.shape[1]
    keys_part = block_kv[0].reshape(block_kv.shape[1], heads_here, queries.shape[2])
    vals_part = block_kv[1].reshape(block_kv.shape[1], heads_here, queries.shape[2])
    scores = (
        jnp.einsum("thc,shc->ths", queries, keys_part, preferred_element_type=jnp.float32) * factor
    )
    highest = jnp.maximum(running, jnp.max(scores, axis=2))
    expon = jnp.exp(scores - highest[:, :, None])
    denoms = jnp.sum(expon, axis=2)
    weights = expon.astype(jnp.bfloat16)
    accum = jnp.einsum("ths,shc->thc", weights, vals_part, preferred_element_type=jnp.float32)
    return (highest, denoms, accum)


def start_totals(rows, heads_count):
    return (
        jnp.full((rows, heads_count), -1e30, jnp.float32),
        jnp.zeros((rows, heads_count), jnp.float32),
        jnp.zeros((rows, heads_count, HEAD_DIM), jnp.float32),
    )


def on_device(tokens, ln_gain, w_qkv, w_out):
    tok_rows = tokens.shape[0]
    whole = lax.all_gather(tokens, "tp", axis=1, tiled=True)
    values = whole.astype(jnp.float32)
    average = jnp.mean(values, axis=1, keepdims=True)
    second = jnp.mean(values * values, axis=1, keepdims=True)
    normed = (
        (values - average)
        * lax.rsqrt(second - average * average + 1e-06)
        * ln_gain.astype(jnp.float32)
    ).astype(jnp.bfloat16)
    projected = jnp.einsum("td,jdc->jtc", normed, w_qkv, preferred_element_type=jnp.float32).astype(
        jnp.bfloat16
    )
    heads_here = w_qkv.shape[2] // HEAD_DIM
    factor = HEAD_DIM ** (-0.5)
    queries = projected[0].reshape(tok_rows, heads_here, HEAD_DIM)
    keys_vals = projected[1:3]
    initial = start_totals(tok_rows, heads_here)
    final = attend_block(
        initial, queries, lax.all_gather(keys_vals, "seq", axis=1, tiled=True), factor
    )
    context = (
        (final[2] / final[1][:, :, None])
        .reshape(tok_rows, heads_here * HEAD_DIM)
        .astype(jnp.bfloat16)
    )
    summed = lax.psum_scatter(
        lax.dot_general(
            w_out, context, (((0,), (1,)), ((), ())), preferred_element_type=jnp.float32
        ).astype(jnp.bfloat16),
        "tp",
        scatter_dimension=0,
        tiled=True,
    ).astype(jnp.float32)
    return (tokens.astype(jnp.float32) + summed.T).astype(jnp.bfloat16)


def solution(mesh):
    in_specs = (P("seq", "tp"), P(), P(None, None, "tp"), P("tp", None))
    out_specs = P("seq", "tp")
    n, cores = mesh.shape["seq"], mesh.shape["tp"]

    def run(tokens, ln_gain, w_qkv, w_out):
        heads = w_qkv.shape[2] // HEAD_DIM
        if cores == 2 and heads * cores == n and n % 8 == 0 and tokens.shape[0] % n == 0:
            return half_per_layer(n, tokens, ln_gain, w_qkv, w_out)
        return on_device(tokens, ln_gain, w_qkv, w_out)

    return jax.shard_map(run, mesh=mesh, in_specs=in_specs, out_specs=out_specs, check_vma=False)
```

```python
import functools
import math

import jax
import jax.numpy as jnp
from jax import lax
from jax.experimental import pallas as pl
from jax.experimental.pallas import tpu as pltpu
from jax.sharding import PartitionSpec as P

HEAD_DIM = 128
MESH = pl.DeviceIdType.MESH


def remote(src, dst, send, recv, seq, tp):
    return pltpu.make_async_remote_copy(
        src_ref=src, dst_ref=dst, send_sem=send, recv_sem=recv, device_id=(seq, tp), device_id_type=MESH
    )


def put(src, dst, send, recv, seq, tp, own):
    @pl.when(own)
    def _():
        pltpu.make_async_copy(src, dst, recv).start()

    @pl.when(jnp.logical_not(own))
    def _():
        remote(src, dst, send, recv, seq, tp).start()


def barrier_wait(barrier, count):
    pl.semaphore_wait(barrier, count)


def half_kernel(
    n, heads, tok, gain_ref, w_qkv, w_out, out,
    pair, far, normed, first, wbuf, wout, xq, xk, xv, yq, yk, yv, q_all, k_all, v_all, acc, top, s0, s1, ctx, held, sent, came,
    kept, res, gain, lsem, swap, wsem, xsem, osem, qsend, qrecv, fsend, frecv, csend, crecv, psem,
):
    me, core = lax.axis_index("seq"), lax.axis_index("tp")
    other = 1 - core
    rows, feats = pair.shape[1], pair.shape[2]
    plane, near = n // 4, n // 2
    groups = plane // 2
    piece = rows // groups
    layer, spot = me // plane, lax.rem(me, plane)
    side, inner = me // near, lax.rem(me // plane, 2)
    central = inner != side
    mate = (2 - side) * plane + spot
    lane = lax.rem(me, 2)
    head = side * plane + spot
    bf, f32 = jnp.bfloat16, jnp.float32

    barrier = pltpu.get_barrier_semaphore()

    def greet(i, carry):
        there = lax.rem(2 * me + core + i, 2 * n)
        pl.semaphore_signal(barrier, inc=1, device_id=(there // 2, lax.rem(there, 2)), device_id_type=MESH)
        return carry

    lax.fori_loop(1, 2 * n, greet, 0)
    mine = pltpu.make_async_copy(tok, pair.at[core], lsem.at[0])
    mine.start()
    trade = remote(tok, pair.at[core], swap.at[0], swap.at[1], me, other)

    def cut(c):
        return pl.ds(c * piece, piece)

    kind = 1 - central.astype(jnp.int32)

    def across(c, half, src=None):
        src = normed.at[half, cut(c)] if src is None else src
        return remote(src, far.at[kind, half, cut(c)], xsem.at[0, kind, c, half], xsem.at[1, kind, c, half], mate, core)

    def inside(which, c, half):
        ref = far.at[which, half, cut(c)]
        return remote(ref, ref, xsem.at[2, which, c, half], xsem.at[3, which, c, half], me, other)

    def sends_x(when):
        return jnp.logical_and(core == inner, when)

    def wcopy(j):
        at = pl.ds(pl.multiple_of(side * plane * HEAD_DIM, HEAD_DIM), plane * HEAD_DIM)
        return pltpu.make_async_copy(w_qkv.at[j, :, at], wbuf.at[j], wsem.at[j])

    for j in range(3):
        wcopy(j).start()
    fetch_out = pltpu.make_async_copy(w_out, wout, lsem.at[1])
    fetch_out.start()
    gain[...] = gain_ref[...].astype(f32).reshape(1, 2 * feats)
    acc[...] = jnp.zeros_like(acc)
    top[...] = jnp.full_like(top, -1e30)
    v_all[:, HEAD_DIM:, :] = jnp.ones((v_all.shape[0], v_all.shape[1] - HEAD_DIM, v_all.shape[2]), bf)
    barrier_wait(barrier, 2 * n - 1)
    trade.start()

    @pl.when(sends_x(central))
    def _():
        across(0, core, tok.at[cut(0)]).start()

    mine.wait()
    trade.wait()

    @pl.when(sends_x(central))
    def _():
        across(0, other, pair.at[other, cut(0)]).start()

    step = 32

    def normalize(src, dst, count):
        def norm(i, carry):
            to = pl.ds(pl.multiple_of(i * step, step), step)
            a = src[0, to, :].astype(f32)
            b = src[1, to, :].astype(f32)
            average = (jnp.sum(a, axis=1, keepdims=True) + jnp.sum(b, axis=1, keepdims=True)) / (2 * feats)
            second = (jnp.sum(a * a, axis=1, keepdims=True) + jnp.sum(b * b, axis=1, keepdims=True)) / (2 * feats)
            scale = lax.rsqrt(second - average * average + 1e-06)
            dst[0, to, :] = ((a - average) * scale * gain[0:1, :feats]).astype(bf)
            dst[1, to, :] = ((b - average) * scale * gain[0:1, feats:]).astype(bf)
            return carry

        lax.fori_loop(0, count // step, norm, 0, unroll=2)

    factor = HEAD_DIM ** (-0.5) * math.log2(math.e)

    def spots(block, u, i):
        if block == 0:
            k_at = u * plane + i
            return q_all.at[i], k_all.at[k_at], v_all.at[k_at, pl.ds(0, HEAD_DIM)]
        k_at = 2 * plane + 2 * (block - 1) + u
        at = pl.ds(pl.multiple_of(i * piece, piece), piece)
        return q_all.at[plane + block - 1, at], k_all.at[k_at, at], v_all.at[k_at, pl.ds(0, HEAD_DIM), at]

    def staged(block, h):
        if block == 0:
            return xq.at[h], xk.at[h], xv.at[h]
        return yq.at[block - 1, h], yk.at[block - 1, h], yv.at[block - 1, h]

    def moves(block, h, j):
        chip = side * near + core * plane + h
        own = jnp.logical_and(chip == me, core == lane)
        i = lax.rem(me, near) // 2 if block == 0 else spot // 2
        src, dst = staged(block, h)[j], spots(block, lane, i)[j]
        return (src, dst, qsend.at[block, h, j], qrecv.at[block, i, j], chip, lane), own

    def deliver(block, h, j):
        args, own = moves(block, h, j)
        put(*args, own)

    def delivered(block, h, j):
        args, own = moves(block, h, j)

        @pl.when(jnp.logical_not(own))
        def _():
            remote(*args).wait_send()

    def project(block, src):
        for j in range(3):
            if block == 0:
                wcopy(j).wait()
            got = jnp.dot(src[0], wbuf[j, :feats], preferred_element_type=f32)
            got = got + jnp.dot(src[1], wbuf[j, feats:], preferred_element_type=f32)
            if j == 0:
                got = got * factor
            for h in range(plane):
                part = got[:, h * HEAD_DIM : (h + 1) * HEAD_DIM]
                staged(block, h)[j][...] = (part.T if j == 2 else part).astype(bf)
            for turn in range(plane):
                deliver(block, lax.rem(spot + turn, plane), j)

    def landing(which):
        return core == (side if which == 0 else 1 - side)

    def relay(w):
        which, c = w // groups, w % groups

        @pl.when(jnp.logical_and(central, landing(which)))
        def _():
            for half in range(2):
                ref = far.at[which, half, cut(c)]
                remote(ref, ref, xsem.at[0, which, c, half], xsem.at[1, which, c, half], mate, core).wait_recv()
                inside(which, c, half).start()

    def wave(w):
        which, c = w // groups, w % groups

        @pl.when(central)
        def _():
            @pl.when(jnp.logical_not(landing(which)))
            def _():
                for half in range(2):
                    inside(which, c, half).wait_recv()

            if w == 0:
                normalize(far.at[0, :, cut(0)], first, piece)
                project(1, first)
            else:
                project(w + 1, far.at[which, :, cut(c)])

    def wait_block(block, i):
        for j, (src, dst) in enumerate(zip(staged(block, 0), spots(block, core, i))):
            remote(src, dst, qsend.at[block, 0, j], qrecv.at[block, i, j], me, other).wait_recv()

    def share(slot, u, way):
        at = u * plane + slot if way == 0 else 2 * plane + 2 * slot + u
        sem = slot if way == 0 else plane + slot
        k_ref, v_ref = k_all.at[at], v_all.at[at, pl.ds(0, HEAD_DIM)]
        return (
            remote(k_ref, k_ref, fsend.at[sem, 0], frecv.at[sem, 0], me, other),
            remote(v_ref, v_ref, fsend.at[sem, 1], frecv.at[sem, 1], me, other),
        )

    def pass_on(slot, way):
        for copy in share(slot, core, way):
            copy.start()

    def from_other(slot, way):
        for copy in share(slot, other, way):
            copy.wait_recv()

    def segment(rects):
        total = sum(nq * nk for _, nq, _, nk in rects)

        def find(t):
            spot_q = spot_k = None
            before = 0
            for q0, nq, k0, nk in rects:
                a = q0 + (t - before) // nk
                b = k0 + lax.rem(t - before, nk)
                if spot_q is None:
                    spot_q, spot_k = a, b
                else:
                    spot_q = jnp.where(t >= before, a, spot_q)
                    spot_k = jnp.where(t >= before, b, spot_k)
                before += nq * nk
            return spot_q, spot_k

        def score(t, s):
            a, b = find(t)
            s[...] = lax.dot_general(k_all[b], q_all[a], (((1,), (1,)), ((), ())), preferred_element_type=f32)

        def weigh(t, s):
            a, b = find(t)
            now = s[...]
            was = top[a]
            high = jnp.maximum(was, jnp.max(now, axis=0, keepdims=True))
            p = jnp.exp2((now - high).astype(bf))
            add = jnp.dot(v_all[b], p, preferred_element_type=f32)
            acc[a] = acc[a] * jnp.exp2(was - high) + add
            top[a] = high

        score(jnp.int32(0), s0)

        def body(i, carry):
            t = 2 * i
            score(t + 1, s1)
            weigh(t, s0)
            score(jnp.minimum(t + 2, total - 1), s0)
            weigh(t + 1, s1)
            return carry

        lax.fori_loop(0, total // 2, body, 0)
        if total % 2:
            weigh(jnp.int32(total - 1), s0)

    def place(l, at):
        return held.at[at, pl.ds(pl.multiple_of(l * HEAD_DIM, HEAD_DIM), HEAD_DIM)]

    def returns(b):
        if b < plane:
            s = side * near + 2 * b + core
            own = jnp.logical_and(s == me, inner == core)
            return [((ctx.at[b], place(head, pl.ds(0, rows)), csend.at[b, 0], crecv.at[head, 0], s, inner), own)]
        w = b - plane
        which, c = w // groups, w % groups
        home = (2 - side) if which == 0 else 3 * (1 - side)
        return [
            ((ctx.at[b, cut(i)], place(head, cut(c)), csend.at[b, i], crecv.at[head, c], home * plane + 2 * i + core, inner), None)
            for i in range(groups)
        ]

    def finish(start, count):
        def one(b, carry):
            t = acc[b]
            ctx[b] = (t[:HEAD_DIM] / t[HEAD_DIM : HEAD_DIM + 1]).T.astype(bf)
            return carry

        lax.fori_loop(start, start + count, one, 0)
        for b in range(start, start + count):
            for args, own in returns(b):
                if own is None:
                    remote(*args).start()
                else:
                    put(*args, own)

    normalize(pair, normed, rows)

    @pl.when(sends_x(central))
    def _():
        for c in range(1, groups):
            for half in range(2):
                across(c, half).start()

    project(0, normed)

    relay(0)
    wave(0)
    here, there = groups * inner, groups * (1 - inner)
    for k in range(groups):
        wait_block(0, here + k)
        pass_on(here + k, 0)

    segment([(here, groups, core * plane + here, groups)])
    relay(1)
    for k in range(groups):
        wait_block(0, there + k)
        pass_on(there + k, 0)

    @pl.when(sends_x(jnp.logical_not(central)))
    def _():
        for c in range(groups):
            for half in range(2):
                across(c, half).start()
    segment([(here, groups, core * plane + there, groups)])
    wave(1)
    segment([(there, groups, core * plane, plane)])
    relay(2)
    for k in range(plane):
        from_other(k, 0)
    segment([(0, plane, other * plane, plane)])
    wave(2)

    def take(w):
        for i in range(groups):
            wait_block(w + 1, i)
        pass_on(w, 1)

    base = 2 * plane
    take(0)
    segment([(plane, 1, 0, base)])
    from_other(0, 1)
    relay(3)
    segment([(plane, 1, base, 2), (0, plane, base, 2)])
    wave(3)
    take(1)
    segment([(plane + 1, 1, 0, base + 2), (plane, 2, base + 2 + core, 1)])
    from_other(1, 1)
    segment([(plane, 2, base + 2 + other, 1), (0, plane, base + 2, 2)])
    take(2)
    segment([(plane + 2, 1, 0, base + 4), (plane, 3, base + 4 + core, 1)])
    from_other(2, 1)
    take(3)
    segment([(plane, 3, base + 4 + other, 1), (plane, 3, base + 6 + core, 1)])
    from_other(3, 1)
    segment([(plane, 3, base + 6 + other, 1)])
    finish(plane, plane - 1)
    segment([(plane + 3, 1, 0, base + 8)])
    finish(plane + 3, 1)
    for half in range(2):
        segment([(half * groups, groups, base + 4, 4)])
        finish(half * groups, groups)

    fetch_out.wait()
    for k in range(plane):
        l = side * plane + k
        remote(ctx.at[0], place(l, pl.ds(0, rows)), csend.at[0, 0], crecv.at[l, 0], me, other).wait_recv()

    def product(half, c):
        at = pl.ds(pl.multiple_of(half * feats, feats), feats)
        return jnp.dot(held[c * piece : (c + 1) * piece, :], wout[:, at], preferred_element_type=f32)

    def hand(c):
        return remote(sent.at[c], came.at[c], psem.at[0, c], psem.at[1, c], me, other)

    def leave(c):
        return pltpu.make_async_copy(res.at[cut(c)], out.at[cut(c)], osem.at[c])

    for c in range(groups):
        for k in range(plane):
            l = (1 - side) * plane + k
            remote(ctx.at[0, cut(c)], place(l, cut(c)), csend.at[0, 0], crecv.at[l, c], me, other).wait_recv()
        sent[c] = product(other, c).astype(bf)
        hand(c).start()
        kept[c * piece : (c + 1) * piece, :] = product(core, c)

    for c in range(groups):
        hand(c).wait_recv()
        at = slice(c * piece, (c + 1) * piece)
        res[at, :] = (pair[core, at, :].astype(f32) + (kept[at, :] + came[c].astype(f32))).astype(bf)
        leave(c).start()

    for h in range(plane):
        for j in range(3):
            delivered(0, h, j)

    @pl.when(central)
    def _():
        for block in range(1, plane + 1):
            for h in range(plane):
                for j in range(3):
                    delivered(block, h, j)
        for which in range(2):
            lands = core == (side if which == 0 else 1 - side)

            @pl.when(lands)
            def _():
                for c in range(groups):
                    for half in range(2):
                        inside(which, c, half).wait_send()

    for slot in range(plane):
        for way in range(2):
            for copy in share(slot, core, way):
                copy.wait_send()

    @pl.when(core == inner)
    def _():
        for c in range(groups):
            for half in range(2):
                across(c, half).wait_send()

    for b in range(2 * plane):
        for args, own in returns(b):
            if own is None:
                remote(*args).wait_send()
            else:

                @pl.when(jnp.logical_not(own))
                def _():
                    remote(*args).wait_send()

    for c in range(groups):
        hand(c).wait_send()
        leave(c).wait()


def half_per_layer(n, tokens, ln_gain, w_qkv, w_out):
    rows, feats = tokens.shape
    heads = w_qkv.shape[2] // HEAD_DIM
    plane = n // 4
    groups = plane // 2
    piece = rows // groups
    bf, f32 = jnp.bfloat16, jnp.float32
    dma = pltpu.SemaphoreType.DMA
    chunks, blocks = 4 * plane, 2 * plane
    extra = HEAD_DIM + 16
    vmem = pltpu.VMEM
    hbm = pl.BlockSpec(memory_space=pltpu.HBM)
    return pl.pallas_call(
        functools.partial(half_kernel, n, heads),
        out_shape=jax.ShapeDtypeStruct((rows, feats), bf),
        in_specs=[hbm, pl.BlockSpec(memory_space=pltpu.VMEM), hbm, hbm],
        out_specs=hbm,
        scratch_shapes=[
            vmem((2, rows, feats), bf),
            vmem((2, 2, rows, feats), bf),
            vmem((2, rows, feats), bf),
            vmem((2, piece, feats), bf),
            vmem((3, 2 * feats, plane * HEAD_DIM), bf),
            vmem(w_out.shape, bf),
            vmem((plane, rows, HEAD_DIM), bf),
            vmem((plane, rows, HEAD_DIM), bf),
            vmem((plane, HEAD_DIM, rows), bf),
            vmem((plane, plane, piece, HEAD_DIM), bf),
            vmem((plane, plane, piece, HEAD_DIM), bf),
            vmem((plane, plane, HEAD_DIM, piece), bf),
            vmem((blocks, rows, HEAD_DIM), bf),
            vmem((chunks, rows, HEAD_DIM), bf),
            vmem((chunks, extra, rows), bf),
            vmem((blocks, extra, rows), f32),
            vmem((blocks, 1, rows), f32),
            vmem((rows, rows), f32),
            vmem((rows, rows), f32),
            vmem((blocks, rows, HEAD_DIM), bf),
            vmem((rows, heads * HEAD_DIM), bf),
            vmem((groups, piece, feats), bf),
            vmem((groups, piece, feats), bf),
            vmem((rows, feats), f32),
            vmem((rows, feats), bf),
            vmem((1, 2 * feats), f32),
            dma((2,)), dma((2,)), dma((3,)), dma((4, 2, groups, 2)), dma((groups,)),
            dma((plane + 1, plane, 3)), dma((plane + 1, plane, 3)), dma((blocks, 2)), dma((blocks, 2)),
            dma((blocks, groups)), dma((heads, groups)), dma((2, groups)),
        ],
        compiler_params=pltpu.CompilerParams(collective_id=0, has_side_effects=True, vmem_limit_bytes=60 * 1024 * 1024),
        name="sublayer",
    )(tokens, ln_gain, w_qkv, w_out)


def attend_block(totals, queries, block_kv, factor):
    running, denoms, accum = totals
    heads_here = queries.shape[1]
    keys_part = block_kv[0].reshape(block_kv.shape[1], heads_here, queries.shape[2])
    vals_part = block_kv[1].reshape(block_kv.shape[1], heads_here, queries.shape[2])
    scores = (
        jnp.einsum("thc,shc->ths", queries, keys_part, preferred_element_type=jnp.float32) * factor
    )
    highest = jnp.maximum(running, jnp.max(scores, axis=2))
    expon = jnp.exp(scores - highest[:, :, None])
    denoms = jnp.sum(expon, axis=2)
    weights = expon.astype(jnp.bfloat16)
    accum = jnp.einsum("ths,shc->thc", weights, vals_part, preferred_element_type=jnp.float32)
    return (highest, denoms, accum)


def start_totals(rows, heads_count):
    return (
        jnp.full((rows, heads_count), -1e30, jnp.float32),
        jnp.zeros((rows, heads_count), jnp.float32),
        jnp.zeros((rows, heads_count, HEAD_DIM), jnp.float32),
    )


def on_device(tokens, ln_gain, w_qkv, w_out):
    tok_rows = tokens.shape[0]
    whole = lax.all_gather(tokens, "tp", axis=1, tiled=True)
    values = whole.astype(jnp.float32)
    average = jnp.mean(values, axis=1, keepdims=True)
    second = jnp.mean(values * values, axis=1, keepdims=True)
    normed = (
        (values - average)
        * lax.rsqrt(second - average * average + 1e-06)
        * ln_gain.astype(jnp.float32)
    ).astype(jnp.bfloat16)
    projected = jnp.einsum("td,jdc->jtc", normed, w_qkv, preferred_element_type=jnp.float32).astype(
        jnp.bfloat16
    )
    heads_here = w_qkv.shape[2] // HEAD_DIM
    factor = HEAD_DIM ** (-0.5)
    queries = projected[0].reshape(tok_rows, heads_here, HEAD_DIM)
    keys_vals = projected[1:3]
    initial = start_totals(tok_rows, heads_here)
    final = attend_block(
        initial, queries, lax.all_gather(keys_vals, "seq", axis=1, tiled=True), factor
    )
    context = (
        (final[2] / final[1][:, :, None])
        .reshape(tok_rows, heads_here * HEAD_DIM)
        .astype(jnp.bfloat16)
    )
    summed = lax.psum_scatter(
        lax.dot_general(
            w_out, context, (((0,), (1,)), ((), ())), preferred_element_type=jnp.float32
        ).astype(jnp.bfloat16),
        "tp",
        scatter_dimension=0,
        tiled=True,
    ).astype(jnp.float32)
    return (tokens.astype(jnp.float32) + summed.T).astype(jnp.bfloat16)


def solution(mesh):
    in_specs = (P("seq", "tp"), P(), P(None, None, "tp"), P("tp", None))
    out_specs = P("seq", "tp")
    n, cores = mesh.shape["seq"], mesh.shape["tp"]

    def run(tokens, ln_gain, w_qkv, w_out):
        heads = w_qkv.shape[2] // HEAD_DIM
        if cores == 2 and heads * cores == n and n % 8 == 0 and tokens.shape[0] % n == 0:
            return half_per_layer(n, tokens, ln_gain, w_qkv, w_out)
        return on_device(tokens, ln_gain, w_qkv, w_out)

    return jax.shard_map(run, mesh=mesh, in_specs=in_specs, out_specs=out_specs, check_vma=False)
```

```python
import functools
import math

import jax
import jax.numpy as jnp
from jax import lax
from jax.experimental import pallas as pl
from jax.experimental.pallas import tpu as pltpu
from jax.sharding import PartitionSpec as P

HEAD_DIM = 128
MESH = pl.DeviceIdType.MESH


def remote(src, dst, send, recv, seq, tp):
    return pltpu.make_async_remote_copy(
        src_ref=src, dst_ref=dst, send_sem=send, recv_sem=recv, device_id=(seq, tp), device_id_type=MESH
    )


def put(src, dst, send, recv, seq, tp, own):
    @pl.when(own)
    def _():
        pltpu.make_async_copy(src, dst, recv).start()

    @pl.when(jnp.logical_not(own))
    def _():
        remote(src, dst, send, recv, seq, tp).start()


def barrier_wait(barrier, count):
    pl.semaphore_wait(barrier, count)


def half_kernel(
    n, heads, tok, gain_ref, w_qkv, w_out, out,
    pair, far, normed, first, wbuf, wout, xq, xk, xv, yq, yk, yv, q_all, k_all, v_all, acc, top, s0, s1, ctx, held, sent, came,
    kept, gone, res, gain, lsem, swap, wsem, xsem, osem, qsend, qrecv, fsend, frecv, csend, crecv, psem,
):
    me, core = lax.axis_index("seq"), lax.axis_index("tp")
    other = 1 - core
    rows, feats = pair.shape[1], pair.shape[2]
    plane, near = n // 4, n // 2
    groups = plane // 2
    piece = rows // groups
    layer, spot = me // plane, lax.rem(me, plane)
    side, inner = me // near, lax.rem(me // plane, 2)
    central = inner != side
    mate = (2 - side) * plane + spot
    lane = lax.rem(me, 2)
    head = side * plane + spot
    bf, f32 = jnp.bfloat16, jnp.float32

    barrier = pltpu.get_barrier_semaphore()

    def greet(i, carry):
        there = lax.rem(2 * me + core + i, 2 * n)
        pl.semaphore_signal(barrier, inc=1, device_id=(there // 2, lax.rem(there, 2)), device_id_type=MESH)
        return carry

    lax.fori_loop(1, 2 * n, greet, 0)
    mine = pltpu.make_async_copy(tok, pair.at[core], lsem.at[0])
    mine.start()
    trade = remote(tok, pair.at[core], swap.at[0], swap.at[1], me, other)

    def cut(c):
        return pl.ds(c * piece, piece)

    kind = 1 - central.astype(jnp.int32)

    def across(c, half, src=None):
        src = normed.at[half, cut(c)] if src is None else src
        return remote(src, far.at[kind, half, cut(c)], xsem.at[0, kind, c, half], xsem.at[1, kind, c, half], mate, core)

    def inside(which, c, half):
        ref = far.at[which, half, cut(c)]
        return remote(ref, ref, xsem.at[2, which, c, half], xsem.at[3, which, c, half], me, other)

    def sends_x(when):
        return jnp.logical_and(core == inner, when)

    def wcopy(j):
        at = pl.ds(pl.multiple_of(side * plane * HEAD_DIM, HEAD_DIM), plane * HEAD_DIM)
        return pltpu.make_async_copy(w_qkv.at[j, :, at], wbuf.at[j], wsem.at[j])

    for j in range(3):
        wcopy(j).start()
    fetch_out = pltpu.make_async_copy(w_out, wout, lsem.at[1])
    fetch_out.start()
    gain[...] = gain_ref[...].astype(f32).reshape(1, 2 * feats)
    acc[...] = jnp.zeros_like(acc)
    top[...] = jnp.full_like(top, -1e30)
    v_all[:, HEAD_DIM:, :] = jnp.ones((v_all.shape[0], v_all.shape[1] - HEAD_DIM, v_all.shape[2]), bf)
    barrier_wait(barrier, 2 * n - 1)
    trade.start()

    @pl.when(sends_x(central))
    def _():
        across(0, core, tok.at[cut(0)]).start()

    mine.wait()
    trade.wait()

    @pl.when(sends_x(central))
    def _():
        across(0, other, pair.at[other, cut(0)]).start()

    step = 32

    def normalize(src, dst, count):
        def norm(i, carry):
            to = pl.ds(pl.multiple_of(i * step, step), step)
            a = src[0, to, :].astype(f32)
            b = src[1, to, :].astype(f32)
            average = (jnp.sum(a, axis=1, keepdims=True) + jnp.sum(b, axis=1, keepdims=True)) / (2 * feats)
            second = (jnp.sum(a * a, axis=1, keepdims=True) + jnp.sum(b * b, axis=1, keepdims=True)) / (2 * feats)
            scale = lax.rsqrt(second - average * average + 1e-06)
            dst[0, to, :] = ((a - average) * scale * gain[0:1, :feats]).astype(bf)
            dst[1, to, :] = ((b - average) * scale * gain[0:1, feats:]).astype(bf)
            return carry

        lax.fori_loop(0, count // step, norm, 0, unroll=2)

    factor = HEAD_DIM ** (-0.5) * math.log2(math.e)

    def spots(block, u, i):
        if block == 0:
            k_at = u * plane + i
            return q_all.at[i], k_all.at[k_at], v_all.at[k_at, pl.ds(0, HEAD_DIM)]
        k_at = 2 * plane + 2 * (block - 1) + u
        at = pl.ds(pl.multiple_of(i * piece, piece), piece)
        return q_all.at[plane + block - 1, at], k_all.at[k_at, at], v_all.at[k_at, pl.ds(0, HEAD_DIM), at]

    def staged(block, h):
        if block == 0:
            return xq.at[h], xk.at[h], xv.at[h]
        return yq.at[block - 1, h], yk.at[block - 1, h], yv.at[block - 1, h]

    def moves(block, h, j):
        chip = side * near + core * plane + h
        own = jnp.logical_and(chip == me, core == lane)
        i = lax.rem(me, near) // 2 if block == 0 else spot // 2
        src, dst = staged(block, h)[j], spots(block, lane, i)[j]
        return (src, dst, qsend.at[block, h, j], qrecv.at[block, i, j], chip, lane), own

    def deliver(block, h, j):
        args, own = moves(block, h, j)
        put(*args, own)

    def delivered(block, h, j):
        args, own = moves(block, h, j)

        @pl.when(jnp.logical_not(own))
        def _():
            remote(*args).wait_send()

    def project(block, src):
        for j in range(3):
            if block == 0:
                wcopy(j).wait()
            got = jnp.dot(src[0], wbuf[j, :feats], preferred_element_type=f32)
            got = got + jnp.dot(src[1], wbuf[j, feats:], preferred_element_type=f32)
            if j == 0:
                got = got * factor
            for h in range(plane):
                part = got[:, h * HEAD_DIM : (h + 1) * HEAD_DIM]
                staged(block, h)[j][...] = (part.T if j == 2 else part).astype(bf)
            for turn in range(plane):
                deliver(block, lax.rem(spot + turn, plane), j)

    def landing(which):
        return core == (side if which == 0 else 1 - side)

    def relay(w):
        which, c = w // groups, w % groups

        @pl.when(jnp.logical_and(central, landing(which)))
        def _():
            for half in range(2):
                ref = far.at[which, half, cut(c)]
                remote(ref, ref, xsem.at[0, which, c, half], xsem.at[1, which, c, half], mate, core).wait_recv()
                inside(which, c, half).start()

    def wave(w):
        which, c = w // groups, w % groups

        @pl.when(central)
        def _():
            @pl.when(jnp.logical_not(landing(which)))
            def _():
                for half in range(2):
                    inside(which, c, half).wait_recv()

            if w == 0:
                normalize(far.at[0, :, cut(0)], first, piece)
                project(1, first)
            else:
                project(w + 1, far.at[which, :, cut(c)])

    def wait_block(block, i):
        for j, (src, dst) in enumerate(zip(staged(block, 0), spots(block, core, i))):
            remote(src, dst, qsend.at[block, 0, j], qrecv.at[block, i, j], me, other).wait_recv()

    def share(slot, u, way):
        at = u * plane + slot if way == 0 else 2 * plane + 2 * slot + u
        sem = slot if way == 0 else plane + slot
        k_ref, v_ref = k_all.at[at], v_all.at[at, pl.ds(0, HEAD_DIM)]
        return (
            remote(k_ref, k_ref, fsend.at[sem, 0], frecv.at[sem, 0], me, other),
            remote(v_ref, v_ref, fsend.at[sem, 1], frecv.at[sem, 1], me, other),
        )

    def pass_on(slot, way):
        for copy in share(slot, core, way):
            copy.start()

    def from_other(slot, way):
        for copy in share(slot, other, way):
            copy.wait_recv()

    def segment(rects):
        total = sum(nq * nk for _, nq, _, nk in rects)

        def find(t):
            spot_q = spot_k = None
            before = 0
            for q0, nq, k0, nk in rects:
                a = q0 + (t - before) // nk
                b = k0 + lax.rem(t - before, nk)
                if spot_q is None:
                    spot_q, spot_k = a, b
                else:
                    spot_q = jnp.where(t >= before, a, spot_q)
                    spot_k = jnp.where(t >= before, b, spot_k)
                before += nq * nk
            return spot_q, spot_k

        def score(t, s):
            a, b = find(t)
            s[...] = lax.dot_general(k_all[b], q_all[a], (((1,), (1,)), ((), ())), preferred_element_type=f32)

        def weigh(t, s):
            a, b = find(t)
            now = s[...]
            was = top[a]
            high = jnp.maximum(was, jnp.max(now, axis=0, keepdims=True))
            p = jnp.exp2((now - high).astype(bf))
            add = jnp.dot(v_all[b], p, preferred_element_type=f32)
            acc[a] = acc[a] * jnp.exp2(was - high) + add
            top[a] = high

        score(jnp.int32(0), s0)

        def body(i, carry):
            t = 2 * i
            score(t + 1, s1)
            weigh(t, s0)
            score(jnp.minimum(t + 2, total - 1), s0)
            weigh(t + 1, s1)
            return carry

        lax.fori_loop(0, total // 2, body, 0)
        if total % 2:
            weigh(jnp.int32(total - 1), s0)

    def place(l, at):
        return held.at[at, pl.ds(pl.multiple_of(l * HEAD_DIM, HEAD_DIM), HEAD_DIM)]

    def returns(b):
        if b < plane:
            s = side * near + 2 * b + core
            own = jnp.logical_and(s == me, inner == core)
            return [((ctx.at[b], place(head, pl.ds(0, rows)), csend.at[b, 0], crecv.at[head, 0], s, inner), own)]
        w = b - plane
        which, c = w // groups, w % groups
        home = (2 - side) if which == 0 else 3 * (1 - side)
        return [
            ((ctx.at[b, cut(i)], place(head, cut(c)), csend.at[b, i], crecv.at[head, c], home * plane + 2 * i + core, inner), None)
            for i in range(groups)
        ]

    def finish(start, count):
        def one(b, carry):
            t = acc[b]
            ctx[b] = (t[:HEAD_DIM] / t[HEAD_DIM : HEAD_DIM + 1]).T.astype(bf)
            return carry

        lax.fori_loop(start, start + count, one, 0)
        for b in range(start, start + count):
            for args, own in returns(b):
                if own is None:
                    remote(*args).start()
                else:
                    put(*args, own)

    normalize(pair, normed, rows)

    @pl.when(sends_x(central))
    def _():
        for c in range(1, groups):
            for half in range(2):
                across(c, half).start()

    project(0, normed)

    relay(0)
    wave(0)
    here, there = groups * inner, groups * (1 - inner)
    for k in range(groups):
        wait_block(0, here + k)
        pass_on(here + k, 0)

    segment([(here, groups, core * plane + here, groups)])
    relay(1)
    for k in range(groups):
        wait_block(0, there + k)
        pass_on(there + k, 0)

    @pl.when(sends_x(jnp.logical_not(central)))
    def _():
        for c in range(groups):
            for half in range(2):
                across(c, half).start()
    segment([(here, groups, core * plane + there, groups)])
    wave(1)
    segment([(there, groups, core * plane, plane)])
    relay(2)
    for k in range(plane):
        from_other(k, 0)
    segment([(0, plane, other * plane, plane)])
    wave(2)

    def take(w):
        for i in range(groups):
            wait_block(w + 1, i)
        pass_on(w, 1)

    base = 2 * plane
    take(0)
    segment([(plane, 1, 0, base)])
    from_other(0, 1)
    relay(3)
    segment([(plane, 1, base, 2), (0, plane, base, 2)])
    wave(3)
    take(1)
    segment([(plane + 1, 1, 0, base + 2), (plane, 2, base + 2 + core, 1)])
    from_other(1, 1)
    segment([(plane, 2, base + 2 + other, 1), (0, plane, base + 2, 2)])
    take(2)
    segment([(plane + 2, 1, 0, base + 4), (plane, 3, base + 4 + core, 1)])
    from_other(2, 1)
    take(3)
    segment([(plane, 3, base + 4 + other, 1), (plane, 3, base + 6 + core, 1)])
    from_other(3, 1)
    segment([(plane, 3, base + 6 + other, 1)])
    finish(plane, plane - 1)
    segment([(plane + 3, 1, 0, base + 8)])
    finish(plane + 3, 1)
    for half in range(2):
        segment([(half * groups, groups, base + 4, 4)])
        finish(half * groups, groups)

    fetch_out.wait()
    deep = plane * HEAD_DIM

    def product(part, half, c):
        k_at = pl.ds(pl.multiple_of(part * deep, deep), deep)
        at = pl.ds(pl.multiple_of(half * feats, feats), feats)
        return jnp.dot(held[cut(c), k_at], wout[k_at, at], preferred_element_type=f32)

    def hand(c):
        return remote(sent.at[c], came.at[c], psem.at[0, c], psem.at[1, c], me, other)

    def leave(c):
        return pltpu.make_async_copy(res.at[cut(c)], out.at[cut(c)], osem.at[c])

    for c in range(groups):
        for k in range(plane):
            l = (1 - side) * plane + k
            remote(ctx.at[0, cut(c)], place(l, cut(c)), csend.at[0, 0], crecv.at[l, c], me, other).wait_recv()
        gone[cut(c), :] = product(1 - side, other, c)
        kept[cut(c), :] = product(1 - side, core, c) + pair[core, cut(c), :].astype(f32)
    for k in range(plane):
        l = side * plane + k
        remote(ctx.at[0], place(l, pl.ds(0, rows)), csend.at[0, 0], crecv.at[l, 0], me, other).wait_recv()
    for c in range(groups):
        sent[c] = (gone[cut(c), :] + product(side, other, c)).astype(bf)
        hand(c).start()
    for c in range(groups):
        kept[cut(c), :] = kept[cut(c), :] + product(side, core, c)
    for c in range(groups):
        hand(c).wait_recv()
        res[cut(c), :] = (kept[cut(c), :] + came[c].astype(f32)).astype(bf)
        leave(c).start()

    for h in range(plane):
        for j in range(3):
            delivered(0, h, j)

    @pl.when(central)
    def _():
        for block in range(1, plane + 1):
            for h in range(plane):
                for j in range(3):
                    delivered(block, h, j)
        for which in range(2):
            lands = core == (side if which == 0 else 1 - side)

            @pl.when(lands)
            def _():
                for c in range(groups):
                    for half in range(2):
                        inside(which, c, half).wait_send()

    for slot in range(plane):
        for way in range(2):
            for copy in share(slot, core, way):
                copy.wait_send()

    @pl.when(core == inner)
    def _():
        for c in range(groups):
            for half in range(2):
                across(c, half).wait_send()

    for b in range(2 * plane):
        for args, own in returns(b):
            if own is None:
                remote(*args).wait_send()
            else:

                @pl.when(jnp.logical_not(own))
                def _():
                    remote(*args).wait_send()

    for c in range(groups):
        hand(c).wait_send()
        leave(c).wait()


def half_per_layer(n, tokens, ln_gain, w_qkv, w_out):
    rows, feats = tokens.shape
    heads = w_qkv.shape[2] // HEAD_DIM
    plane = n // 4
    groups = plane // 2
    piece = rows // groups
    bf, f32 = jnp.bfloat16, jnp.float32
    dma = pltpu.SemaphoreType.DMA
    chunks, blocks = 4 * plane, 2 * plane
    extra = HEAD_DIM + 16
    vmem = pltpu.VMEM
    hbm = pl.BlockSpec(memory_space=pltpu.HBM)
    return pl.pallas_call(
        functools.partial(half_kernel, n, heads),
        out_shape=jax.ShapeDtypeStruct((rows, feats), bf),
        in_specs=[hbm, pl.BlockSpec(memory_space=pltpu.VMEM), hbm, hbm],
        out_specs=hbm,
        scratch_shapes=[
            vmem((2, rows, feats), bf),
            vmem((2, 2, rows, feats), bf),
            vmem((2, rows, feats), bf),
            vmem((2, piece, feats), bf),
            vmem((3, 2 * feats, plane * HEAD_DIM), bf),
            vmem(w_out.shape, bf),
            vmem((plane, rows, HEAD_DIM), bf),
            vmem((plane, rows, HEAD_DIM), bf),
            vmem((plane, HEAD_DIM, rows), bf),
            vmem((plane, plane, piece, HEAD_DIM), bf),
            vmem((plane, plane, piece, HEAD_DIM), bf),
            vmem((plane, plane, HEAD_DIM, piece), bf),
            vmem((blocks, rows, HEAD_DIM), bf),
            vmem((chunks, rows, HEAD_DIM), bf),
            vmem((chunks, extra, rows), bf),
            vmem((blocks, extra, rows), f32),
            vmem((blocks, 1, rows), f32),
            vmem((rows, rows), f32),
            vmem((rows, rows), f32),
            vmem((blocks, rows, HEAD_DIM), bf),
            vmem((rows, heads * HEAD_DIM), bf),
            vmem((groups, piece, feats), bf),
            vmem((groups, piece, feats), bf),
            vmem((rows, feats), f32),
            vmem((rows, feats), f32),
            vmem((rows, feats), bf),
            vmem((1, 2 * feats), f32),
            dma((2,)), dma((2,)), dma((3,)), dma((4, 2, groups, 2)), dma((groups,)),
            dma((plane + 1, plane, 3)), dma((plane + 1, plane, 3)), dma((blocks, 2)), dma((blocks, 2)),
            dma((blocks, groups)), dma((heads, groups)), dma((2, groups)),
        ],
        compiler_params=pltpu.CompilerParams(collective_id=0, has_side_effects=True, vmem_limit_bytes=60 * 1024 * 1024),
        name="sublayer",
    )(tokens, ln_gain, w_qkv, w_out)


def attend_block(totals, queries, block_kv, factor):
    running, denoms, accum = totals
    heads_here = queries.shape[1]
    keys_part = block_kv[0].reshape(block_kv.shape[1], heads_here, queries.shape[2])
    vals_part = block_kv[1].reshape(block_kv.shape[1], heads_here, queries.shape[2])
    scores = (
        jnp.einsum("thc,shc->ths", queries, keys_part, preferred_element_type=jnp.float32) * factor
    )
    highest = jnp.maximum(running, jnp.max(scores, axis=2))
    expon = jnp.exp(scores - highest[:, :, None])
    denoms = jnp.sum(expon, axis=2)
    weights = expon.astype(jnp.bfloat16)
    accum = jnp.einsum("ths,shc->thc", weights, vals_part, preferred_element_type=jnp.float32)
    return (highest, denoms, accum)


def start_totals(rows, heads_count):
    return (
        jnp.full((rows, heads_count), -1e30, jnp.float32),
        jnp.zeros((rows, heads_count), jnp.float32),
        jnp.zeros((rows, heads_count, HEAD_DIM), jnp.float32),
    )


def on_device(tokens, ln_gain, w_qkv, w_out):
    tok_rows = tokens.shape[0]
    whole = lax.all_gather(tokens, "tp", axis=1, tiled=True)
    values = whole.astype(jnp.float32)
    average = jnp.mean(values, axis=1, keepdims=True)
    second = jnp.mean(values * values, axis=1, keepdims=True)
    normed = (
        (values - average)
        * lax.rsqrt(second - average * average + 1e-06)
        * ln_gain.astype(jnp.float32)
    ).astype(jnp.bfloat16)
    projected = jnp.einsum("td,jdc->jtc", normed, w_qkv, preferred_element_type=jnp.float32).astype(
        jnp.bfloat16
    )
    heads_here = w_qkv.shape[2] // HEAD_DIM
    factor = HEAD_DIM ** (-0.5)
    queries = projected[0].reshape(tok_rows, heads_here, HEAD_DIM)
    keys_vals = projected[1:3]
    initial = start_totals(tok_rows, heads_here)
    final = attend_block(
        initial, queries, lax.all_gather(keys_vals, "seq", axis=1, tiled=True), factor
    )
    context = (
        (final[2] / final[1][:, :, None])
        .reshape(tok_rows, heads_here * HEAD_DIM)
        .astype(jnp.bfloat16)
    )
    summed = lax.psum_scatter(
        lax.dot_general(
            w_out, context, (((0,), (1,)), ((), ())), preferred_element_type=jnp.float32
        ).astype(jnp.bfloat16),
        "tp",
        scatter_dimension=0,
        tiled=True,
    ).astype(jnp.float32)
    return (tokens.astype(jnp.float32) + summed.T).astype(jnp.bfloat16)


def solution(mesh):
    in_specs = (P("seq", "tp"), P(), P(None, None, "tp"), P("tp", None))
    out_specs = P("seq", "tp")
    n, cores = mesh.shape["seq"], mesh.shape["tp"]

    def run(tokens, ln_gain, w_qkv, w_out):
        heads = w_qkv.shape[2] // HEAD_DIM
        if cores == 2 and heads * cores == n and n % 8 == 0 and tokens.shape[0] % n == 0:
            return half_per_layer(n, tokens, ln_gain, w_qkv, w_out)
        return on_device(tokens, ln_gain, w_qkv, w_out)

    return jax.shard_map(run, mesh=mesh, in_specs=in_specs, out_specs=out_specs, check_vma=False)
```
